32 devices in a mesh: batch: 2 (over core), expert: 16 (over z, y, x).
Axes of the slice: x: 2, y: 2, z: 4, core: 2. Of those that a mesh axis runs over, the one named last changes fastest.
Arguments:
- section_inputs: bfloat16 [4, 4096, 2048], P(None, ('batch', 'expert')), may hold values from -6 to 6
- adjoint_end: bfloat16 [4096, 2048], P(('batch', 'expert')), may hold values from -6 to 6
- gate_probs: float32 [4, 4096, 2], P(None, ('batch', 'expert')), may hold values from 0.2 to 1
- expert_ids: int32 [4, 4096, 2], P(None, ('batch', 'expert')), may hold values from 0 to 15, all different within a row
- norm_gain: float32 [2048], replicated, may hold values from 0.1 to 1.9
- gate_weight: bfloat16 [16, 2048, 384], P('expert'), may hold values from -0.125 to 0.125
- up_weight: bfloat16 [16, 2048, 384], P('expert'), may hold values from -0.125 to 0.125
- down_weight: bfloat16 [16, 2048, 384], P('expert'), may hold values from -0.3125 to 0.3125
Outputs:
- adjoint_start: float32 [4096, 2048], P(('batch', 'expert'))
- gate_grad: float32 [16, 2048, 384], P('expert', 'batch')
- up_grad: float32 [16, 2048, 384], P('expert', 'batch')
- down_grad: float32 [16, 2048, 384], P('expert', 'batch')
The draws below stay inside these ranges and needn't reach their ends.
Inputs may be any that keep to these rules, and one draw needn't show every extreme that they name: `expert_ids`: the 2 experts of a token in a section differ.
All inputs are finite; a program needn't handle non-finite values.
Results may differ from the reference program's by a relative error of at most 0.0095.
Values may be sent and summed in bfloat16 or wider, within the bound.
No kernel may reach another device: no remote copies, remote signals or barrier semaphores. Data moves between devices by JAX's collectives and lax.ppermute only.
A program may use at most 128 MiB of HBM per device.

```python
import jax
import jax.numpy as jnp
from jax import lax

D = 2048
FF_WIN = 384
TOK_DEV = 128
SECTIONS = 4
TOP = 2
EXPERTS = 16
CAP = 16
TOKENS = 4096
N_BATCH = 2
N_EXPERT = 16


def block_scale(rng, extent, shards, least, high):
    level = 1.0
    for position, parts in shards:
        steps = jax.random.uniform(jax.random.fold_in(jax.random.fold_in(rng, 6), position), (parts,), jnp.float32, least / len(shards), high / len(shards))
        level = level * jnp.repeat(jnp.exp(steps), extent[position] // parts).reshape((-1,) + (1,) * (len(extent) - 1 - position))
    return level


def picks_of(own_key, rows, amount, top, lift):
    order = jax.random.permutation(jax.random.fold_in(own_key, 1), amount)
    pull = order
    for power in range(3):
        pull = pull * pull // amount
    pull = pull * lift // amount
    chance = jax.random.randint(jax.random.fold_in(own_key, 2), (rows, amount), 0, 4096) + pull
    fixed_rows = jax.random.permutation(jax.random.fold_in(own_key, 3), rows)[jnp.arange(amount) % rows]
    chance = jnp.where(jnp.arange(rows)[:, None] == fixed_rows[None, :], 1 << 14, chance)
    priority = chance * amount + jnp.arange(amount)
    return lax.top_k(priority.astype(jnp.int32), top)[1].astype(jnp.int32)


def gaussian(stream_key, dims, scale, most, split=(), kind=jnp.bfloat16):
    result = scale * jax.random.normal(stream_key, dims, jnp.float32)
    if split:
        result = result * block_scale(stream_key, dims, split, -0.22, 0.18)
    return jnp.clip(result, -most, most).astype(kind)


def setup_inputs(seed: int = 0) -> dict:
    seeds = jax.random.split(jax.random.key(seed), 9)
    return {
        "section_inputs": gaussian(seeds[0], (SECTIONS, TOKENS, D), 1.0, 6.0, ((1, 32),)),
        "adjoint_end": gaussian(seeds[1], (TOKENS, D), 1.0, 6.0, ((0, 32),)),
        "gate_probs": jnp.clip(0.2 + 0.8 * jax.random.uniform(seeds[2], (SECTIONS, TOKENS, TOP), jnp.float32) ** block_scale(seeds[2], (SECTIONS, TOKENS, TOP), ((1, 32),), -0.2, 0.2), 0.2, 1.0),
        "expert_ids": picks_of(seeds[3], SECTIONS * TOKENS, EXPERTS, TOP, 2048).reshape((SECTIONS, TOKENS, TOP)),
        "norm_gain": jnp.clip(1.0 + 0.18 * jax.random.normal(seeds[4], (D,), jnp.float32), 0.1, 1.9),
        "gate_weight": gaussian(seeds[5], (EXPERTS, D, FF_WIN), D ** -0.5, 0.125, ((0, 16),)),
        "up_weight": gaussian(seeds[6], (EXPERTS, D, FF_WIN), D ** -0.5, 0.125, ((0, 16),)),
        "down_weight": gaussian(seeds[7], (EXPERTS, D, FF_WIN), FF_WIN ** -0.5, 0.3125, ((0, 16),)),
    }


EPS = 1e-06
STEP = 1.0
ALONG_END = (1.0 / 6.0, 1.0 / 3.0, 1.0 / 3.0, 1.0 / 6.0)
ALONG_NEXT = (0.5, 0.5, 1.0, 0.0)

def contract_rows(left_op, right_op):
    return lax.dot_general(left_op, right_op, (((0,), (0,)), ((), ())), preferred_element_type=jnp.float32)

def contract_cols(left_op, right_op):
    return lax.dot_general(left_op, right_op, (((1,), (1,)), ((), ())), preferred_element_type=jnp.float32)

def normalize(inputs, gain_row):
    values = inputs.astype(jnp.float32)
    inverse = lax.rsqrt(lax.optimization_barrier(jnp.mean(values * values, axis=-1, keepdims=True)) + EPS)
    return ((values * inverse * gain_row).astype(jnp.bfloat16), values, inverse)

def norm_back(values, inverse, gain_row, cotangent):
    weighted = gain_row * cotangent
    return inverse * weighted - values * (inverse * inverse * inverse) * lax.optimization_barrier(jnp.mean(values * weighted, axis=-1, keepdims=True))

def expert_back(rows_in, rows_cot, gate_mat, up_mat, down_mat):
    gate_pre = jnp.dot(rows_in, gate_mat, preferred_element_type=jnp.float32)
    upward = jnp.dot(rows_in, up_mat, preferred_element_type=jnp.float32)
    logistic = jax.nn.sigmoid(gate_pre)
    active = gate_pre * logistic
    hidden = (active * upward).astype(jnp.bfloat16)
    grad_hidden = jnp.dot(rows_cot, down_mat, preferred_element_type=jnp.float32)
    grad_gate = (grad_hidden * upward * (logistic * (1.0 + gate_pre * (1.0 - logistic)))).astype(jnp.bfloat16)
    grad_up = (grad_hidden * active).astype(jnp.bfloat16)
    rows_back = (contract_cols(grad_gate, gate_mat) + contract_cols(grad_up, up_mat)).astype(jnp.bfloat16)
    return (rows_back, contract_rows(rows_in, grad_gate), contract_rows(rows_in, grad_up), contract_rows(rows_cot, hidden))

def slots(flat_ids):
    hit_table = (flat_ids[:, None] == jnp.arange(EXPERTS, dtype=jnp.int32)[None, :]).astype(jnp.int32)
    before = jnp.cumsum(hit_table, axis=0) - hit_table
    return lax.optimization_barrier(jnp.sum(before * hit_table, axis=1)).astype(jnp.int32)

def reference(section_inputs, adjoint_end, gate_probs, expert_ids, norm_gain, gate_weight, up_weight, down_weight):
    gain_row = norm_gain.astype(jnp.float32)
    places = N_EXPERT * CAP
    source = jnp.arange(N_EXPERT, dtype=jnp.int32)[None, :, None]
    groups = jnp.arange(N_BATCH, dtype=jnp.int32)[:, None, None]
    end_adjoint = adjoint_end.astype(jnp.float32)
    adjoint_start = end_adjoint
    following = jnp.zeros_like(end_adjoint)
    sum_gate = jnp.zeros((EXPERTS, D, FF_WIN), jnp.float32)
    sum_up = jnp.zeros((EXPERTS, D, FF_WIN), jnp.float32)
    sum_down = jnp.zeros((EXPERTS, D, FF_WIN), jnp.float32)
    for number in (3, 2, 1, 0):
        normed, values, inverse = normalize(section_inputs[number], gain_row)
        cotangent = STEP * ALONG_END[number] * end_adjoint + STEP * ALONG_NEXT[number] * following
        rows_cot = (gate_probs[number][:, :, None] * cotangent[:, None, :]).astype(jnp.bfloat16)
        chosen = expert_ids[number].astype(jnp.int32).reshape(N_BATCH, N_EXPERT, TOK_DEV * TOP)
        slot_index = jax.vmap(jax.vmap(slots))(chosen).reshape(N_BATCH, N_EXPERT, TOK_DEV, TOP)
        chosen = chosen.reshape(N_BATCH, N_EXPERT, TOK_DEV, TOP)
        target = jnp.where(slot_index < CAP, source[..., None] * CAP + slot_index, places).astype(jnp.int32)
        normed_tok = normed.reshape(N_BATCH, N_EXPERT, TOK_DEV, D)
        cot_tok = rows_cot.reshape(N_BATCH, N_EXPERT, TOK_DEV, TOP, D)
        held_in = jnp.zeros((N_BATCH, EXPERTS, places, D), jnp.bfloat16)
        held_cot = jnp.zeros((N_BATCH, EXPERTS, places, D), jnp.bfloat16)
        for column in range(TOP):
            held_in = held_in.at[groups, chosen[..., column], target[..., column]].set(normed_tok, mode='drop')
            held_cot = held_cot.at[groups, chosen[..., column], target[..., column]].set(cot_tok[..., column, :], mode='drop')

        def per_expert(packed):
            rows_in, rows_c, gate_mat, up_mat, down_mat = packed
            back_list = []
            part_gate = jnp.zeros((D, FF_WIN), jnp.float32)
            part_up = jnp.zeros((D, FF_WIN), jnp.float32)
            part_down = jnp.zeros((D, FF_WIN), jnp.float32)
            for group_idx in range(N_BATCH):
                rows_back, one_gate, one_up, one_down = expert_back(rows_in[group_idx], rows_c[group_idx], gate_mat, up_mat, down_mat)
                back_list.append(rows_back)
                part_gate = part_gate + one_gate
                part_up = part_up + one_up
                part_down = part_down + one_down
            return (jnp.stack(back_list), part_gate, part_up, part_down)
        back_rows, part_gate, part_up, part_down = lax.map(per_expert, (jnp.transpose(held_in, (1, 0, 2, 3)), jnp.transpose(held_cot, (1, 0, 2, 3)), gate_weight, up_weight, down_weight))
        sum_gate = sum_gate + part_gate
        sum_up = sum_up + part_up
        sum_down = sum_down + part_down
        back_rows = jnp.transpose(back_rows, (1, 0, 2, 3))
        grad_in = jnp.zeros((N_BATCH, N_EXPERT, TOK_DEV, D), jnp.float32)
        for column in range(TOP):
            picked = back_rows.at[groups, chosen[..., column], target[..., column]].get(mode='fill', fill_value=0)
            grad_in = grad_in + picked.astype(jnp.float32)
        following = norm_back(values, inverse, gain_row, grad_in.reshape(TOKENS, D))
        adjoint_start = adjoint_start + following
    return (adjoint_start, sum_gate, sum_up, sum_down)
```

```python
import functools

import jax
import jax.numpy as jnp
from jax import lax
from jax.experimental import pallas as pl
from jax.experimental.pallas import tpu as pltpu
from jax.sharding import PartitionSpec as P

SECTIONS = 4
TOP = 2

EPS = 1e-06
STEP = 1.0
ALONG_END = (1.0 / 6.0, 1.0 / 3.0, 1.0 / 3.0, 1.0 / 6.0)
ALONG_NEXT = (0.5, 0.5, 1.0, 0.0)
CHUNK = 256


def contract_rows(left_op, right_op):
    return lax.dot_general(
        left_op, right_op, (((0,), (0,)), ((), ())), preferred_element_type=jnp.float32
    )


def contract_cols(left_op, right_op):
    return lax.dot_general(
        left_op, right_op, (((1,), (1,)), ((), ())), preferred_element_type=jnp.float32
    )


def mxu(left_op, right_op):
    return jnp.dot(left_op, right_op, preferred_element_type=jnp.float32)


def places_of(ids, experts, capacity):
    tokens = ids.shape[1]
    each = lax.broadcasted_iota(jnp.int32, (experts, tokens), 0)
    hits = [each == ids[j : j + 1, :] for j in range(TOP)]
    count = sum(h.astype(jnp.float32) for h in hits).astype(jnp.bfloat16)
    earlier = lax.broadcasted_iota(jnp.int32, (tokens, tokens), 0) < lax.broadcasted_iota(
        jnp.int32, (tokens, tokens), 1
    )
    before = mxu(count, earlier.astype(jnp.float32).astype(jnp.bfloat16))
    place = lax.broadcasted_iota(jnp.int32, (experts * capacity, tokens), 0)
    masks = []
    for j in range(TOP):
        slot = jnp.sum(jnp.where(hits[j], before, 0.0), axis=0, keepdims=True).astype(jnp.int32)
        target = jnp.where(slot < capacity, ids[j : j + 1, :] * capacity + slot, -1)
        masks.append(place == target)
    return masks


def join(masks):
    return sum(m.astype(jnp.float32) for m in masks)


def chunks_of(width):
    return width // CHUNK


def cols(step):
    return pl.ds(pl.multiple_of(step * CHUNK, CHUNK), CHUNK)


def inverse_norm(u_ref):
    tokens, width = u_ref.shape

    def body(step, total):
        part = u_ref[:, cols(step)].astype(jnp.float32)
        return total + jnp.sum(part * part, axis=1, keepdims=True)

    total = lax.fori_loop(0, chunks_of(width), body, jnp.zeros((tokens, 1), jnp.float32))
    return lax.rsqrt(total / width + EPS)


def pack_in_kernel(experts, capacity, ids_ref, u_ref, gain_ref, sent_ref):
    width = u_ref.shape[1]
    pick = join(places_of(ids_ref[...], experts, capacity)).astype(jnp.bfloat16)
    inverse = inverse_norm(u_ref)

    def body(step, _):
        part = u_ref[:, cols(step)].astype(jnp.float32)
        normed = (part * inverse * gain_ref[:, cols(step)]).astype(jnp.bfloat16)
        sent_ref[:, cols(step)] = mxu(pick, normed).astype(jnp.bfloat16)
        return 0

    lax.fori_loop(0, chunks_of(width), body, 0)


def pack_cot(masks, probs, cotangent):
    pick = join(masks).astype(jnp.bfloat16)
    high = cotangent.astype(jnp.bfloat16)
    low = (cotangent - high.astype(jnp.float32)).astype(jnp.bfloat16)
    return (probs * (mxu(pick, high) + mxu(pick, low))).astype(jnp.bfloat16)


def place_probs(masks, probs):
    return sum(
        jnp.sum(jnp.where(masks[j], probs[j : j + 1, :], 0.0), axis=1, keepdims=True)
        for j in range(TOP)
    )


def first_cot_kernel(experts, capacity, along, ids_ref, probs_ref, end_ref, sent_ref):
    width = end_ref.shape[1]
    masks = places_of(ids_ref[...], experts, capacity)
    probs = place_probs(masks, probs_ref[...])

    def body(step, _):
        cotangent = along * end_ref[:, cols(step)].astype(jnp.float32)
        sent_ref[:, cols(step)] = pack_cot(masks, probs, cotangent)
        return 0

    lax.fori_loop(0, chunks_of(width), body, 0)


def combine_kernel(
    experts, capacity, along, ids_ref, next_ids_ref, next_probs_ref, back_ref, u_ref, gain_ref,
    end_ref, total_ref, *out
):
    sent_ref, sum_ref, weighted_ref = out if along else (None, *out)
    tokens, width = u_ref.shape
    pick = join(places_of(ids_ref[...], experts, capacity)).T.astype(jnp.bfloat16)

    def first(step, carry):
        square, cross = carry
        part = u_ref[:, cols(step)].astype(jnp.float32)
        weighted = gain_ref[:, cols(step)] * mxu(pick, back_ref[:, cols(step)])
        weighted_ref[:, cols(step)] = weighted
        return (
            square + jnp.sum(part * part, axis=1, keepdims=True),
            cross + jnp.sum(part * weighted, axis=1, keepdims=True),
        )

    zero = jnp.zeros((tokens, 1), jnp.float32)
    square, cross = lax.fori_loop(0, chunks_of(width), first, (zero, zero))
    inverse = lax.rsqrt(square / width + EPS)
    scale = inverse * inverse * inverse * (cross / width)
    if along:
        masks = places_of(next_ids_ref[...], experts, capacity)
        probs = place_probs(masks, next_probs_ref[...])

    def second(step, _):
        part = u_ref[:, cols(step)].astype(jnp.float32)
        following = inverse * weighted_ref[:, cols(step)] - part * scale
        sum_ref[:, cols(step)] = total_ref[:, cols(step)].astype(jnp.float32) + following
        if along:
            end = end_ref[:, cols(step)].astype(jnp.float32)
            sent_ref[:, cols(step)] = pack_cot(
                masks, probs, along[0] * end + along[1] * following
            )
        return 0

    lax.fori_loop(0, chunks_of(width), second, 0)


def call(kernel, outs, scratch=(), flops=0, moved=0):
    return pl.pallas_call(
        kernel,
        out_shape=outs,
        scratch_shapes=list(scratch),
        cost_estimate=pl.CostEstimate(flops=flops, bytes_accessed=moved, transcendentals=0),
        compiler_params=pltpu.CompilerParams(vmem_limit_bytes=24 * 2**20),
    )


def expert_front(rows_in, gate_mat, up_mat):
    gate_pre = mxu(rows_in, gate_mat)
    upward = mxu(rows_in, up_mat)
    logistic = jax.nn.sigmoid(gate_pre)
    active = gate_pre * logistic
    hidden = (active * upward).astype(jnp.bfloat16)
    slope = upward * (logistic * (1.0 + gate_pre * (1.0 - logistic)))
    return (slope, active, hidden)


def expert_back(rows_cot, slope, active, gate_mat, up_mat, down_mat):
    grad_hidden = mxu(rows_cot, down_mat)
    grad_gate = (grad_hidden * slope).astype(jnp.bfloat16)
    grad_up = (grad_hidden * active).astype(jnp.bfloat16)
    rows_back = (contract_cols(grad_gate, gate_mat) + contract_cols(grad_up, up_mat)).astype(
        jnp.bfloat16
    )
    return (rows_back, grad_gate, grad_up)


def exchange(rows):
    return lax.all_to_all(rows, "expert", split_axis=0, concat_axis=0, tiled=True)


def on_device(
    section_inputs,
    adjoint_end,
    gate_probs,
    expert_ids,
    norm_gain,
    gate_weight,
    up_weight,
    down_weight,
):
    experts = lax.axis_size("expert")
    tokens, width = adjoint_end.shape
    capacity = max(2, TOP * tokens // experts)
    places = experts * capacity
    gate_mat = gate_weight[0]
    up_mat = up_weight[0]
    down_mat = down_weight[0]
    gain = norm_gain.reshape(1, width)
    ids = jnp.transpose(expert_ids, (0, 2, 1))
    probs = jnp.transpose(gate_probs, (0, 2, 1))
    rows = jax.ShapeDtypeStruct((places, width), jnp.bfloat16)
    wide = jax.ShapeDtypeStruct((tokens, width), jnp.float32)
    work = 2 * places * tokens * width

    held_in = {}
    for number in (3, 2, 1, 0):
        sent_in = call(
            functools.partial(pack_in_kernel, experts, capacity), rows, flops=work, moved=3 * 2**19
        )(ids[number], section_inputs[number], gain)
        held_in[number] = exchange(sent_in)
    sent_cot = call(
        functools.partial(first_cot_kernel, experts, capacity, STEP * ALONG_END[3]),
        rows,
        flops=2 * work,
        moved=3 * 2**19,
    )(ids[3], probs[3], adjoint_end)
    kept = []
    total = adjoint_end
    for number in (3, 2, 1, 0):
        slope, active, hidden = expert_front(held_in[number], gate_mat, up_mat)
        held_cot = exchange(sent_cot)
        rows_back, grad_gate, grad_up = expert_back(
            held_cot, slope, active, gate_mat, up_mat, down_mat
        )
        kept.append((held_in[number], held_cot, hidden, grad_gate, grad_up))
        returned = exchange(rows_back)
        following = max(number - 1, 0)
        along = (
            (STEP * ALONG_END[following], STEP * ALONG_NEXT[following]) if number else None
        )
        results = call(
            functools.partial(combine_kernel, experts, capacity, along),
            (rows, wide) if number else (wide,),
            scratch=[pltpu.VMEM((tokens, width), jnp.float32)],
            flops=3 * work,
            moved=6 * 2**20,
        )(
            ids[number], ids[following], probs[following], returned, section_inputs[number],
            gain, adjoint_end, total
        )
        if number:
            sent_cot, total = results
        else:
            (total,) = results
    every_in, every_cot, every_hidden, every_gate, every_up = (
        jnp.concatenate(parts, axis=0) for parts in zip(*kept)
    )
    pairs = ((every_in, every_gate), (every_in, every_up), (every_cot, every_hidden))
    halves = lax.axis_size("batch")
    if halves != 2:
        summed = [
            lax.psum_scatter(contract_rows(*pair), "batch", scatter_dimension=0, tiled=True)
            for pair in pairs
        ]
    else:
        mine = lax.axis_index("batch")
        half = width // halves

        def part(pair, which):
            return contract_rows(
                lax.dynamic_slice_in_dim(pair[0], which * half, half, axis=1), pair[1]
            )

        others = [part(pair, 1 - mine).astype(jnp.bfloat16) for pair in pairs]
        came = [lax.ppermute(other, "batch", [(0, 1), (1, 0)]) for other in others]
        summed = [part(pair, mine) + one.astype(jnp.float32) for pair, one in zip(pairs, came)]
    return (total, summed[0][None], summed[1][None], summed[2][None])


def solution(mesh):
    in_specs = (
        P(None, ("batch", "expert"), None),
        P(("batch", "expert"), None),
        P(None, ("batch", "expert"), None),
        P(None, ("batch", "expert"), None),
        P(),
        P("expert", None, None),
        P("expert", None, None),
        P("expert", None, None),
    )
    out_specs = (
        P(("batch", "expert"), None),
        P("expert", "batch", None),
        P("expert", "batch", None),
        P("expert", "batch", None),
    )
    return jax.shard_map(
        on_device, mesh=mesh, in_specs=in_specs, out_specs=out_specs, check_vma=False
    )
```

```python
import functools

import jax
import jax.numpy as jnp
from jax import lax
from jax.experimental import pallas as pl
from jax.experimental.pallas import tpu as pltpu
from jax.sharding import PartitionSpec as P


SECTIONS = 4
TOP = 2

EPS = 1e-06
STEP = 1.0
ALONG_END = (1.0 / 6.0, 1.0 / 3.0, 1.0 / 3.0, 1.0 / 6.0)
ALONG_NEXT = (0.5, 0.5, 1.0, 0.0)
CHUNK = 512
MOST_PERMUTES = 16


def contract_rows(left_op, right_op):
    return lax.dot_general(
        left_op, right_op, (((0,), (0,)), ((), ())), preferred_element_type=jnp.float32
    )


def contract_cols(left_op, right_op):
    return lax.dot_general(
        left_op, right_op, (((1,), (1,)), ((), ())), preferred_element_type=jnp.float32
    )


def mxu(left_op, right_op):
    return jnp.dot(left_op, right_op, preferred_element_type=jnp.float32)


def places_of(ids, experts, capacity):
    tokens = ids.shape[1]
    each = lax.broadcasted_iota(jnp.int32, (experts, tokens), 0)
    hits = [each == ids[j : j + 1, :] for j in range(TOP)]
    count = sum(h.astype(jnp.float32) for h in hits).astype(jnp.bfloat16)
    earlier = lax.broadcasted_iota(jnp.int32, (tokens, tokens), 0) < lax.broadcasted_iota(
        jnp.int32, (tokens, tokens), 1
    )
    before = mxu(count, earlier.astype(jnp.float32).astype(jnp.bfloat16))
    place = lax.broadcasted_iota(jnp.int32, (experts * capacity, tokens), 0)
    masks = []
    for j in range(TOP):
        slot = jnp.sum(jnp.where(hits[j], before, 0.0), axis=0, keepdims=True).astype(jnp.int32)
        target = jnp.where(slot < capacity, ids[j : j + 1, :] * capacity + slot, -1)
        masks.append(place == target)
    return masks


def join(masks):
    return sum(m.astype(jnp.float32) for m in masks)


def chunks_of(width):
    return [pl.ds(start, CHUNK) for start in range(0, width, CHUNK)]


def fetch(source, target, sem):
    copy = pltpu.make_async_copy(source, target, sem)
    copy.start()
    return copy


def place_probs(masks, probs):
    return sum(
        jnp.sum(jnp.where(masks[j], probs[j : j + 1, :], 0.0), axis=1, keepdims=True)
        for j in range(TOP)
    )


def pack_cot(pick, probs, cotangent):
    high = cotangent.astype(jnp.bfloat16)
    low = (cotangent - high.astype(jnp.float32)).astype(jnp.bfloat16)
    return (probs * mxu(pick, jnp.concatenate([high, low], axis=0))).astype(jnp.bfloat16)


def pick_twice(masks):
    pick = join(masks).astype(jnp.bfloat16)
    return jnp.concatenate([pick, pick], axis=1)


def pack_in_kernel(number, experts, capacity, ids_ref, gain_ref, u_hbm, *rest):
    *sent_hbm, u_ref, sent_ref, sems = rest
    tokens, width = u_ref.shape
    chunks = chunks_of(width)
    arrive = fetch(u_hbm.at[number], u_ref, sems.at[0])
    pick = join(places_of(ids_ref[...], experts, capacity)).astype(jnp.bfloat16)
    arrive.wait()
    square = jnp.zeros((tokens, 1), jnp.float32)
    for at in chunks:
        part = u_ref[:, at].astype(jnp.float32)
        square = square + jnp.sum(part * part, axis=1, keepdims=True)
    inverse = lax.rsqrt(square / width + EPS)
    leaving = []
    for at in chunks:
        normed = (u_ref[:, at].astype(jnp.float32) * inverse * gain_ref[:, at]).astype(jnp.bfloat16)
        sent_ref[:, at] = mxu(pick, normed).astype(jnp.bfloat16)
        start = 0
        for one in sent_hbm:
            rows = pl.ds(start, one.shape[0])
            start += one.shape[0]
            leaving.append(fetch(sent_ref.at[rows, at], one.at[:, at], sems.at[1 + len(leaving)]))
    for copy in leaving:
        copy.wait()


def first_cot_kernel(experts, capacity, along, ids_ref, probs_ref, end_hbm, sent_hbm, end_ref, sent_ref, sems):
    chunks = chunks_of(end_ref.shape[1])
    arrive = fetch(end_hbm, end_ref, sems.at[len(chunks)])
    masks = places_of(ids_ref[...], experts, capacity)
    probs = place_probs(masks, probs_ref[...])
    pick = pick_twice(masks)
    arrive.wait()
    leaving = []
    for step, at in enumerate(chunks):
        sent_ref[:, at] = pack_cot(pick, probs, along * end_ref[:, at].astype(jnp.float32))
        leaving.append(fetch(sent_ref.at[:, at], sent_hbm.at[:, at], sems.at[step]))
    for copy in leaving:
        copy.wait()


def combine_kernel(
    number, experts, capacity, along, ids_ref, next_ids_ref, next_probs_ref, gain_ref, u_hbm,
    base_hbm, back_hbm, out_hbm, u_ref, base_ref, back_ref, weighted_ref, sent_ref, sems
):
    tokens, width = u_ref.shape
    chunks = chunks_of(width)
    many = len(chunks)
    backs = [
        fetch(back_hbm.at[:, at], back_ref.at[:, at], sems.at[step])
        for step, at in enumerate(chunks)
    ]
    arrive_u = fetch(u_hbm.at[number], u_ref, sems.at[many])
    arrive_base = fetch(base_hbm, base_ref, sems.at[many + 1])
    pick = join(places_of(ids_ref[...], experts, capacity)).T.astype(jnp.bfloat16)
    if along:
        masks = places_of(next_ids_ref[...], experts, capacity)
        probs = place_probs(masks, next_probs_ref[...])
        next_pick = pick_twice(masks)
    arrive_u.wait()
    square = jnp.zeros((tokens, 1), jnp.float32)
    cross = jnp.zeros((tokens, 1), jnp.float32)
    for step, at in enumerate(chunks):
        part = u_ref[:, at].astype(jnp.float32)
        square = square + jnp.sum(part * part, axis=1, keepdims=True)
        backs[step].wait()
        weighted = gain_ref[:, at] * mxu(pick, back_ref[:, at])
        weighted_ref[:, at] = weighted
        cross = cross + jnp.sum(part * weighted, axis=1, keepdims=True)
    inverse = lax.rsqrt(square / width + EPS)
    scale = inverse * inverse * inverse * (cross / width)
    arrive_base.wait()
    leaving = []
    for step, at in enumerate(chunks):
        following = inverse * weighted_ref[:, at] - u_ref[:, at].astype(jnp.float32) * scale
        base = base_ref[:, at].astype(jnp.float32)
        if along:
            sent_ref[:, at] = pack_cot(next_pick, probs, along[0] * base + along[1] * following)
            source = sent_ref
        else:
            weighted_ref[:, at] = base + following
            source = weighted_ref
        leaving.append(fetch(source.at[:, at], out_hbm.at[:, at], sems.at[step]))
    for copy in leaving:
        copy.wait()


def regroup_kernel(near_hbm, far_a_hbm, far_b_hbm, *rest):
    *groups, near_ref, far_ref, sems = rest
    half = far_a_hbm.shape[0]
    arriving = [
        fetch(near_hbm, near_ref, sems.at[0]),
        fetch(far_a_hbm, far_ref.at[pl.ds(0, half)], sems.at[1]),
        fetch(far_b_hbm, far_ref.at[pl.ds(half, half)], sems.at[2]),
    ]
    for copy in arriving:
        copy.wait()
    leaving = []
    for far, group in enumerate(groups, 1):
        rows = group.shape[0] // 2
        for part, source in enumerate((near_ref, far_ref)):
            leaving.append(
                fetch(
                    source.at[pl.ds(far * rows, rows)],
                    group.at[pl.ds(part * rows, rows)],
                    sems.at[3 + len(leaving)],
                )
            )
    for copy in leaving:
        copy.wait()


def order_kernel(experts, me_ref, near_hbm, far_hbm, *rest):
    *came, held_ref, sems = rest
    me = me_ref[0, 0]
    rows = held_ref.shape[0] // experts
    copies = []
    for far in range(experts // 2):
        if far:
            sources = [came[far - 1].at[pl.ds(part * rows, rows)] for part in range(2)]
        else:
            sources = [near_hbm.at[pl.ds(0, rows)], far_hbm.at[pl.ds(0, rows)]]
        for part, source in enumerate(sources):
            start = pl.multiple_of((me ^ far ^ (part * experts // 2)) * rows, rows)
            copies.append(
                fetch(source, held_ref.at[pl.ds(start, rows)], sems.at[len(copies)])
            )
    for copy in copies:
        copy.wait()


def experts_kernel(
    slope_ref, active_ref, gate_hbm, up_hbm, down_hbm, cot_hbm, back_hbm, grad_gate_ref,
    grad_up_ref, gate_ref, up_ref, down_ref, cot_ref, back_ref, sems
):
    chunks = chunks_of(cot_ref.shape[1])
    many = len(chunks)
    arriving = []
    for step, at in enumerate(chunks):
        arriving.append(
            (
                fetch(cot_hbm.at[:, at], cot_ref.at[:, at], sems.at[2 * step]),
                fetch(down_hbm.at[at, :], down_ref.at[at, :], sems.at[2 * step + 1]),
            )
        )
    sides = [
        fetch(gate_hbm, gate_ref, sems.at[2 * many]),
        fetch(up_hbm, up_ref, sems.at[2 * many + 1]),
    ]
    grad_hidden = jnp.zeros(slope_ref.shape, jnp.float32)
    for step, at in enumerate(chunks):
        for copy in arriving[step]:
            copy.wait()
        grad_hidden = grad_hidden + mxu(cot_ref[:, at], down_ref[at, :])
    grad_gate = (grad_hidden * slope_ref[...]).astype(jnp.bfloat16)
    grad_up = (grad_hidden * active_ref[...]).astype(jnp.bfloat16)
    grad_gate_ref[...] = grad_gate
    grad_up_ref[...] = grad_up
    for copy in sides:
        copy.wait()
    leaving = []
    for step, at in enumerate(chunks):
        back_ref[:, at] = (
            contract_cols(grad_gate, gate_ref[at, :]) + contract_cols(grad_up, up_ref[at, :])
        ).astype(jnp.bfloat16)
        leaving.append(
            fetch(back_ref.at[:, at], back_hbm.at[:, at], sems.at[2 * many + 2 + step])
        )
    for copy in leaving:
        copy.wait()


VMEM = pl.BlockSpec(memory_space=pltpu.VMEM)
HBM = pl.BlockSpec(memory_space=pltpu.HBM)
SMEM = pl.BlockSpec(memory_space=pltpu.SMEM)


def call(kernel, ins, outs, shapes, scratch, flops):
    return pl.pallas_call(
        kernel,
        in_specs=list(ins),
        out_specs=tuple(outs),
        out_shape=tuple(shapes),
        scratch_shapes=list(scratch),
        cost_estimate=pl.CostEstimate(flops=flops, bytes_accessed=4 * 2**20, transcendentals=0),
    )


def expert_front(rows_in, gate_mat, up_mat):
    gate_pre = mxu(rows_in, gate_mat)
    upward = mxu(rows_in, up_mat)
    logistic = jax.nn.sigmoid(gate_pre)
    active = gate_pre * logistic
    hidden = (active * upward).astype(jnp.bfloat16)
    slope = upward * (logistic * (1.0 + gate_pre * (1.0 - logistic)))
    return lax.optimization_barrier((slope, active, hidden))


def exchange(rows):
    return lax.all_to_all(rows, "expert", split_axis=0, concat_axis=0, tiled=True)


def spread(sent, me, experts):
    near, far_a, far_b = sent
    half = experts // 2
    far = []
    for one in (far_a, far_b):
        far.append(lax.ppermute(one, "expert", [(e, e ^ half) for e in range(experts)]))
    rows = near.shape[0] // half
    width = near.shape[1]
    groups = call(
        regroup_kernel,
        [HBM] * 3,
        [HBM] * (half - 1),
        [jax.ShapeDtypeStruct((2 * rows, width), near.dtype)] * (half - 1),
        [pltpu.VMEM(near.shape, near.dtype)] * 2 + [pltpu.SemaphoreType.DMA((experts + 1,))],
        10**8,
    )(near, *far)
    came = []
    for distance, group in enumerate(groups, 1):
        came.append(
            lax.ppermute(group, "expert", [(e, e ^ distance) for e in range(experts)])
        )
    return call(
        functools.partial(order_kernel, experts),
        [SMEM] + [HBM] * (half + 1),
        [VMEM],
        [jax.ShapeDtypeStruct((2 * near.shape[0], width), near.dtype)],
        [pltpu.SemaphoreType.DMA((experts,))],
        10**8,
    )(me.reshape(1, 1), near, far[0], *came)[0]


def on_device(
    section_inputs,
    adjoint_end,
    gate_probs,
    expert_ids,
    norm_gain,
    gate_weight,
    up_weight,
    down_weight,
):
    experts = lax.axis_size("expert")
    me = lax.axis_index("expert").astype(jnp.int32)
    tokens, width = adjoint_end.shape
    capacity = max(2, TOP * tokens // experts)
    places = experts * capacity
    gate_mat = gate_weight[0]
    up_mat = up_weight[0]
    down_mat = down_weight[0]
    gain = norm_gain.reshape(1, width)
    ids = jnp.transpose(expert_ids, (0, 2, 1))
    probs = jnp.transpose(gate_probs, (0, 2, 1))
    rows = jax.ShapeDtypeStruct((places, width), jnp.bfloat16)
    wide = jax.ShapeDtypeStruct((tokens, width), jnp.float32)
    work = 2 * places * tokens * width
    many = width // CHUNK
    direct = 4 <= experts <= MOST_PERMUTES and experts & (experts - 1) == 0
    last = SECTIONS - 1
    hidden_width = gate_mat.shape[1]
    one_bf = pltpu.VMEM((tokens, width), jnp.bfloat16)
    rows_bf = pltpu.VMEM((places, width), jnp.bfloat16)

    held_in = {}
    for number in range(last, -1, -1):
        aside = direct and number < last
        shares = (2, 4, 4) if aside else (1,)
        sent_in = call(
            functools.partial(pack_in_kernel, number, experts, capacity),
            [VMEM, VMEM, HBM],
            [HBM] * len(shares),
            [jax.ShapeDtypeStruct((places // one, width), jnp.bfloat16) for one in shares],
            [one_bf, rows_bf, pltpu.SemaphoreType.DMA((len(shares) * many + 1,))],
            work,
        )(ids[number] ^ me if aside else ids[number], gain, section_inputs)
        if aside:
            held_in[number] = spread(sent_in, me, experts)
        else:
            held_in[number] = exchange(sent_in[0])
    (sent_cot,) = call(
        functools.partial(first_cot_kernel, experts, capacity, STEP * ALONG_END[last]),
        [VMEM, VMEM, HBM],
        [HBM],
        [rows],
        [one_bf, rows_bf, pltpu.SemaphoreType.DMA((many + 1,))],
        2 * work,
    )(ids[last], probs[last], adjoint_end)
    total = adjoint_end
    summed = None
    for number in range(last, -1, -1):
        slope, active, hidden = expert_front(held_in[number], gate_mat, up_mat)
        held_cot = exchange(sent_cot)
        rows_back, grad_gate, grad_up = call(
            experts_kernel,
            [VMEM] * 2 + [HBM] * 4,
            [HBM, VMEM, VMEM],
            [rows] + [jax.ShapeDtypeStruct((places, hidden_width), jnp.bfloat16)] * 2,
            [pltpu.VMEM((width, hidden_width), jnp.bfloat16)] * 3
            + [rows_bf, rows_bf, pltpu.SemaphoreType.DMA((3 * many + 2,))],
            6 * places * width * hidden_width,
        )(slope, active, gate_mat, up_mat, down_mat, held_cot)
        returned = exchange(rows_back)
        pairs = ((held_in[number], grad_gate), (held_in[number], grad_up), (held_cot, hidden))
        if number:
            parts = [contract_rows(*pair) for pair in pairs]
            summed = parts if summed is None else [a + b for a, b in zip(summed, parts)]
        following = max(number - 1, 0)
        along = (STEP * ALONG_END[following], STEP * ALONG_NEXT[following])

        def combine(along, base, shape):
            return call(
                functools.partial(combine_kernel, number, experts, capacity, along),
                [VMEM] * 4 + [HBM] * 3,
                [HBM],
                [shape],
                [
                    one_bf,
                    pltpu.VMEM((tokens, width), base.dtype),
                    rows_bf,
                    pltpu.VMEM((tokens, width), jnp.float32),
                    rows_bf,
                    pltpu.SemaphoreType.DMA((many + 2,)),
                ],
                3 * work,
            )(
                ids[number], ids[following], probs[following], gain, section_inputs, base,
                returned
            )[0]

        if number:
            sent_cot = combine(along, adjoint_end, rows)
        total = combine(None, total, wide)
    halves = lax.axis_size("batch")
    if halves != 2:
        summed = [
            lax.psum_scatter(one + contract_rows(*pair), "batch", scatter_dimension=0, tiled=True)
            for one, pair in zip(summed, pairs)
        ]
    else:
        mine = lax.axis_index("batch")
        half = width // halves

        def part(one, pair, which):
            left_op = lax.dynamic_slice_in_dim(pair[0], which * half, half, axis=1)
            early = lax.dynamic_slice_in_dim(one, which * half, half, axis=0)
            return early + contract_rows(left_op, pair[1])

        others = [
            part(one, pair, 1 - mine).astype(jnp.bfloat16) for one, pair in zip(summed, pairs)
        ]
        came = [lax.ppermute(other, "batch", [(0, 1), (1, 0)]) for other in others]
        summed = [
            part(one, pair, mine) + two.astype(jnp.float32)
            for one, pair, two in zip(summed, pairs, came)
        ]
    return (total, summed[0][None], summed[1][None], summed[2][None])


def solution(mesh):
    in_specs = (
        P(None, ("batch", "expert"), None),
        P(("batch", "expert"), None),
        P(None, ("batch", "expert"), None),
        P(None, ("batch", "expert"), None),
        P(),
        P("expert", None, None),
        P("expert", None, None),
        P("expert", None, None),
    )
    out_specs = (
        P(("batch", "expert"), None),
        P("expert", "batch", None),
        P("expert", "batch", None),
        P("expert", "batch", None),
    )
    return jax.shard_map(
        on_device, mesh=mesh, in_specs=in_specs, out_specs=out_specs, check_vma=False
    )
```
